32 devices in a mesh: dp: 1 (over z), tp: 4 (over y), sp: 8 (over x, core).
Axes of the slice: x: 4, y: 4, z: 1, core: 2. Of those that a mesh axis runs over, the one named last changes fastest.
The devices are a block of a 4x4x8 slice.
Arguments:
- x: bfloat16 [2048, 5120], P(('dp', 'sp'))
- pos: int32 [2048], P(('dp', 'sp'))
- k_hist: bfloat16 [2, 8192, 8, 128], P(None, ('dp', 'sp'), 'tp')
- v_hist: bfloat16 [2, 8192, 8, 128], P(None, ('dp', 'sp'), 'tp')
- wq: bfloat16 [2, 5120, 5120], P(None, None, 'tp')
- wk: bfloat16 [2, 5120, 1024], P(None, None, 'tp')
- wv: bfloat16 [2, 5120, 1024], P(None, None, 'tp')
- wo: bfloat16 [2, 5120, 5120], P(None, 'tp')
- wg: bfloat16 [2, 5120, 13824], P(None, None, 'tp')
- wu: bfloat16 [2, 5120, 13824], P(None, None, 'tp')
- wd: bfloat16 [2, 13824, 5120], P(None, 'tp')
- g1: bfloat16 [2, 5120], replicated
- g2: bfloat16 [2, 5120], replicated
Outputs:
- output 1: bfloat16 [2048, 5120], P(('dp', 'sp'))
- output 2: bfloat16 [2, 2048, 8, 128], P(None, ('dp', 'sp'), 'tp')
- output 3: bfloat16 [2, 2048, 8, 128], P(None, ('dp', 'sp'), 'tp')
All inputs are finite; a program needn't handle non-finite values.
Results may differ from the reference program's by a relative error of at most 0.02.
Values are sent between devices in bfloat16 or wider.
A program may use at most 768 MiB of HBM per device.

```python
import jax
import jax.numpy as jnp
from jax import lax

D = 5120
HEADS = 40
KV_HEADS = 8
HEAD = 128
FF = 13824
S = 2048
HIST = 8192
LAYERS = 2
QBLK = 32
EPS = 1e-5
ROPE_THETA = 500000.0


def setup_inputs(seed: int = 0, part: int = 0) -> dict:
    key = jax.random.PRNGKey(seed)
    ks = jax.random.split(key, 9)
    kp = jax.random.split(jax.random.fold_in(key, part), 4)
    f32 = jnp.float32

    def w(k, shape, fan_in, gain=1.0):
        return (jax.random.normal(k, shape, f32) * (gain * fan_in ** -0.5)).astype(jnp.bfloat16)

    off = jax.random.randint(kp[1], (), 0, 1024)
    kvshape = (LAYERS, HIST, KV_HEADS, HEAD)
    return {
        'x': jax.random.normal(kp[0], (S, D), f32).astype(jnp.bfloat16),
        'pos': (HIST + off + jnp.arange(S)).astype(jnp.int32),
        'k_hist': jax.random.normal(kp[2], kvshape, f32).astype(jnp.bfloat16),
        'v_hist': jax.random.normal(kp[3], kvshape, f32).astype(jnp.bfloat16),
        'wq': w(ks[0], (LAYERS, D, HEADS * HEAD), D, 3.0),
        'wk': w(ks[1], (LAYERS, D, KV_HEADS * HEAD), D),
        'wv': w(ks[2], (LAYERS, D, KV_HEADS * HEAD), D),
        'wo': w(ks[3], (LAYERS, HEADS * HEAD, D), HEADS * HEAD),
        'wg': w(ks[4], (LAYERS, D, FF), D),
        'wu': w(ks[5], (LAYERS, D, FF), D),
        'wd': w(ks[6], (LAYERS, FF, D), FF),
        'g1': (1.0 + 0.2 * jax.random.normal(ks[7], (LAYERS, D), f32)).astype(jnp.bfloat16),
        'g2': (1.0 + 0.2 * jax.random.normal(ks[8], (LAYERS, D), f32)).astype(jnp.bfloat16),
    }


def rmsnorm(x, g):
    xf = x.astype(jnp.float32)
    r = lax.rsqrt(jnp.mean(xf * xf, axis=-1, keepdims=True) + EPS)
    return (xf * r * g.astype(jnp.float32)).astype(jnp.bfloat16)


def rope(t, pos):
    half = t.shape[-1] // 2
    inv = ROPE_THETA ** (-(jnp.arange(half, dtype=jnp.float32) * (2.0 / t.shape[-1])))
    ang = pos.astype(jnp.float32)[..., None] * inv
    c = jnp.cos(ang)[..., None, :]
    s = jnp.sin(ang)[..., None, :]
    tf = t.astype(jnp.float32)
    t1 = tf[..., :half]
    t2 = tf[..., half:]
    return jnp.concatenate([t1 * c - t2 * s, t2 * c + t1 * s], axis=-1).astype(jnp.bfloat16)


def attention(q, k, v):
    g = HEADS // KV_HEADS
    kf = k.astype(jnp.float32)
    vf = v.astype(jnp.float32)
    qb = q.reshape(S // QBLK, QBLK, KV_HEADS, g, HEAD)
    kidx = jnp.arange(HIST + S)

    def blk(args):
        i, qq = args
        s = jnp.einsum('qkgd,tkd->qkgt', qq.astype(jnp.float32), kf) * HEAD ** -0.5
        qidx = HIST + i * QBLK + jnp.arange(QBLK)
        mask = (kidx[None, :] <= qidx[:, None])[:, None, None, :]
        s = jnp.where(mask, s, -jnp.inf)
        p = jax.nn.softmax(s, axis=-1).astype(jnp.bfloat16)
        o = jnp.einsum('qkgt,tkd->qkgd', p.astype(jnp.float32), vf)
        return o.astype(jnp.bfloat16)

    o = lax.map(blk, (jnp.arange(S // QBLK), qb))
    return o.reshape(S, HEADS * HEAD)


def reference(x, pos, k_hist, v_hist, wq, wk, wv, wo, wg, wu, wd, g1, g2):
    def layer(x, w):
        kh, vh, wq_, wk_, wv_, wo_, wg_, wu_, wd_, g1_, g2_ = w
        h = rmsnorm(x, g1_)
        q = jnp.dot(h, wq_, preferred_element_type=jnp.float32).astype(jnp.bfloat16).reshape(S, HEADS, HEAD)
        k = jnp.dot(h, wk_, preferred_element_type=jnp.float32).astype(jnp.bfloat16).reshape(S, KV_HEADS, HEAD)
        v = jnp.dot(h, wv_, preferred_element_type=jnp.float32).astype(jnp.bfloat16).reshape(S, KV_HEADS, HEAD)
        q = rope(q, pos)
        k = rope(k, pos)
        a = attention(q, jnp.concatenate([kh, k], axis=0), jnp.concatenate([vh, v], axis=0))
        x = x + jnp.dot(a, wo_, preferred_element_type=jnp.float32).astype(jnp.bfloat16)
        h2 = rmsnorm(x, g2_)
        ga = jnp.dot(h2, wg_, preferred_element_type=jnp.float32).astype(jnp.bfloat16)
        up = jnp.dot(h2, wu_, preferred_element_type=jnp.float32).astype(jnp.bfloat16)
        u = (jax.nn.silu(ga.astype(jnp.float32)) * up.astype(jnp.float32)).astype(jnp.bfloat16)
        x = x + jnp.dot(u, wd_, preferred_element_type=jnp.float32).astype(jnp.bfloat16)
        return x, (k, v)

    x, (kn, vn) = lax.scan(layer, x, (k_hist, v_hist, wq, wk, wv, wo, wg, wu, wd, g1, g2))
    return x, kn, vn
```

```python
import functools

import jax
import jax.numpy as jnp
from jax import lax
from jax.experimental import pallas as pl
from jax.experimental.pallas import tpu as pltpu
from jax.sharding import PartitionSpec as P

EPS = 1e-5
ROPE_THETA = 500000.0
LOG2E = 1.4426950408889634
CHUNK = 1024
PARAMS2 = pltpu.CompilerParams(
    dimension_semantics=('arbitrary', 'arbitrary'), vmem_limit_bytes=48 * 1024 * 1024)
PARAMS1 = pltpu.CompilerParams(dimension_semantics=('arbitrary',), vmem_limit_bytes=48 * 1024 * 1024)


def rmsnorm(x, g):
    xf = x.astype(jnp.float32)
    r = lax.rsqrt(jnp.mean(xf * xf, axis=-1, keepdims=True) + EPS)
    return (xf * r * g.astype(jnp.float32)).astype(jnp.bfloat16)


def mm(a, b):
    return jnp.dot(a, b, preferred_element_type=jnp.float32)


def rope_tables(pos, dh):
    half = dh // 2
    inv = ROPE_THETA ** (-(jnp.arange(half, dtype=jnp.float32) * (2.0 / dh)))
    ang = pos.astype(jnp.float32)[:, None] * inv
    c = jnp.cos(ang)
    s = jnp.sin(ang)
    return jnp.concatenate([c, c], axis=-1), jnp.concatenate([-s, s], axis=-1)


def qkv_kernel(nq, h_ref, wq_ref, wk_ref, wv_ref, c_ref, s_ref, q_ref, k_ref, v_ref):
    j = pl.program_id(0)
    dh = c_ref.shape[-1]

    def turn(w_ref, out_ref):
        t = mm(h_ref[...], w_ref[...]).astype(jnp.bfloat16).astype(jnp.float32)
        for i in range(t.shape[-1] // dh):
            th = t[:, i * dh:(i + 1) * dh]
            r = th * c_ref[...] + pltpu.roll(th, dh // 2, 1) * s_ref[...]
            out_ref[:, i * dh:(i + 1) * dh] = r.astype(out_ref.dtype)

    @pl.when(j < nq)
    def _():
        turn(wq_ref, q_ref)

    @pl.when(j == nq)
    def _():
        turn(wk_ref, k_ref)

    @pl.when(j == nq + 1)
    def _():
        v_ref[...] = mm(h_ref[...], wv_ref[...]).astype(v_ref.dtype)


def qkv(h, wq, wk, wv, l, c, s):
    n, d = h.shape
    kvw = wk.shape[-1]
    nq = wq.shape[-1] // kvw
    full = lambda r, w: pl.BlockSpec((r, w), lambda j: (0, 0))
    weight = lambda at: pl.BlockSpec((None, d, kvw), lambda j: (l, 0, at(j)))
    first = lambda j: jnp.minimum(j, nq - 1)
    zero = lambda j: 0
    out = lambda w: jax.ShapeDtypeStruct((n, w), jnp.bfloat16)
    return pl.pallas_call(
        functools.partial(qkv_kernel, nq),
        grid=(nq + 2,),
        in_specs=[full(n, d), weight(first), weight(zero), weight(zero), full(*c.shape), full(*s.shape)],
        out_specs=[pl.BlockSpec((n, kvw), lambda j: (0, first(j))), full(n, kvw), full(n, kvw)],
        out_shape=(out(wq.shape[-1]), out(kvw), out(kvw)),
        compiler_params=PARAMS1,
        cost_estimate=pl.CostEstimate(
            flops=2 * n * d * (nq + 2) * kvw, bytes_accessed=2 * d * (nq + 2) * kvw, transcendentals=0),
        name='qkv',
    )(h, wq, wk, wv, c, s)


def gate_kernel(h_ref, wg_ref, wu_ref, u_ref):
    a = mm(h_ref[...], wg_ref[...]).astype(jnp.bfloat16).astype(jnp.float32)
    b = mm(h_ref[...], wu_ref[...]).astype(jnp.bfloat16).astype(jnp.float32)
    u_ref[...] = (jax.nn.silu(a) * b).astype(u_ref.dtype)


def down_kernel(u_ref, w_ref, o_ref):
    o_ref[...] = mm(u_ref[...], w_ref[...])


def by_columns(kernel, x, ws, l, cols, dtype, name):
    n, d = x.shape
    f = ws[0].shape[-1]
    cols = min(cols, f)
    return pl.pallas_call(
        kernel,
        grid=(pl.cdiv(f, cols),),
        in_specs=[pl.BlockSpec((n, d), lambda j: (0, 0))] + [pl.BlockSpec((None, d, cols), lambda j: (l, 0, j))] * len(ws),
        out_specs=pl.BlockSpec((n, cols), lambda j: (0, j)),
        out_shape=jax.ShapeDtypeStruct((n, f), dtype),
        compiler_params=PARAMS1,
        cost_estimate=pl.CostEstimate(
            flops=2 * len(ws) * n * d * f, bytes_accessed=2 * len(ws) * d * f, transcendentals=0),
        name=name,
    )(x, *ws)


def block(q, k, v, m, l, acc, scale, mask=None):
    s = lax.dot_general(q, k, (((1,), (1,)), ((), ())), preferred_element_type=jnp.float32)
    if mask is not None:
        s = jnp.where(mask, s, -jnp.inf)
    top = jnp.max(s, axis=-1, keepdims=True)
    m_new = top if m is None else jnp.maximum(m, top)
    p = jnp.exp2((s - m_new) * (scale * LOG2E))
    width = v.shape[-1]
    part = p[:, :width]
    for j in range(1, p.shape[-1] // width):
        part = part + p[:, j * width:(j + 1) * width]
    o = lax.dot_general(p.astype(jnp.bfloat16), v, (((1,), (0,)), ((), ())), preferred_element_type=jnp.float32)
    if m is None:
        return m_new, part, o
    a = jnp.exp2((m - m_new) * (scale * LOG2E))
    return m_new, l * a + part, acc * a + o


def hist_kernel(scale, n_whole, n_state, q_ref, *refs):
    state, kv, outs = refs[:n_state], refs[n_state:-3], refs[-3:]
    pairs = [(r, 0, r, r.shape[0] // 2) for r in kv[:n_whole]]
    pairs += [(a, 0, b, 0) for a, b in zip(kv[n_whole::2], kv[n_whole + 1::2])]
    q = q_ref[...]
    m = l = acc = None
    if state:
        m, l, acc = state[0][:, :1], state[1][...], state[2][...]
    for kr, k0, vr, v0 in pairs:
        rows = vr.shape[0] - v0
        m, l, acc = block(q, kr[k0:k0 + rows, :], vr[v0:v0 + rows, :], m, l, acc, scale)
    m_ref, l_ref, o_ref = outs
    m_ref[...] = jnp.broadcast_to(m, m_ref.shape)
    l_ref[...] = l
    o_ref[...] = acc


def new_kernel(scale, idx_ref, q_ref, k_ref, v_ref, m_ref, l_ref, o_ref, out_ref):
    n = q_ref.shape[0]
    q = q_ref[...]
    m, l, acc = m_ref[:, :1], l_ref[...], o_ref[...]
    qpos = idx_ref[0] * n + lax.broadcasted_iota(jnp.int32, (n, CHUNK), 0)
    col = lax.broadcasted_iota(jnp.int32, (n, CHUNK), 1)
    for c in range(k_ref.shape[0] // CHUNK):
        at = slice(c * CHUNK, (c + 1) * CHUNK)
        m, l, acc = block(q, k_ref[at, :], v_ref[at, :], m, l, acc, scale, col + c * CHUNK <= qpos)
    out_ref[...] = (acc / jnp.sum(l, axis=-1, keepdims=True)).astype(out_ref.dtype)


def heads_of(q, dh, kvl):
    g = q.shape[1] // dh // kvl
    return g, pl.BlockSpec((q.shape[0], dh), lambda i, j: (0, i * g + j)), lambda a: pl.BlockSpec((a.shape[0], dh), lambda i, j: (0, i))


def cost(q, n_keys, dh, kvl):
    return pl.CostEstimate(
        flops=8 * q.size * n_keys, bytes_accessed=8 * n_keys * kvl * dh, transcendentals=q.size // dh * n_keys)


def hist_attention(q, state, whole, halves, dh, kvl):
    g, head, keys = heads_of(q, dh, kvl)
    stat = jax.ShapeDtypeStruct(q.shape, jnp.float32)
    return pl.pallas_call(
        functools.partial(hist_kernel, dh ** -0.5, len(whole), len(state)),
        grid=(kvl, g),
        in_specs=[head] * (1 + len(state)) + [keys(a) for a in whole + halves],
        out_specs=[head] * 3,
        out_shape=(stat, stat, stat),
        compiler_params=PARAMS2,
        cost_estimate=cost(q, sum(a.shape[0] for a in whole + halves) // 2, dh, kvl),
        name='hist_attention',
    )(q, *state, *whole, *halves)


def new_attention(idx, q, state, k_all, v_all, dh, kvl):
    g, head, keys = heads_of(q, dh, kvl)
    return pl.pallas_call(
        functools.partial(new_kernel, dh ** -0.5),
        grid=(kvl, g),
        in_specs=[pl.BlockSpec(memory_space=pltpu.SMEM), head, keys(k_all), keys(v_all), head, head, head],
        out_specs=head,
        out_shape=jax.ShapeDtypeStruct(q.shape, jnp.bfloat16),
        compiler_params=PARAMS2,
        cost_estimate=cost(q, k_all.shape[0], dh, kvl),
        name='new_attention',
    )(idx, q, k_all, v_all, *state)


def solution(mesh):
    sp = mesh.shape['sp']
    tp = mesh.shape['tp']
    row = ('dp', 'sp')
    kv_spec = P(None, row, 'tp', None)
    col = P(None, None, 'tp')
    rowsplit = P(None, 'tp', None)
    right = [(i, (i + 2) % sp) for i in range(sp)]
    left = [(i, (i - 2) % sp) for i in range(sp)]
    other = [(i, i ^ 1) for i in range(sp)]

    def to_neighbours(own):
        return lax.ppermute(own, 'sp', right), lax.ppermute(own, 'sp', left)

    def to_far(from_left, from_right):
        half = from_left.shape[0] // 2
        return lax.ppermute(from_left[:half], 'sp', right), lax.ppermute(from_right[half:], 'sp', left)

    def to_other(*blocks):
        return tuple(lax.ppermute(a, 'sp', other) for a in blocks)

    after = lax.optimization_barrier

    def body(x, pos, k_hist, v_hist, wq, wk, wv, wo, wg, wu, wd, g1, g2):
        n, d = x.shape
        layers, nh, kvl, dh = k_hist.shape
        part = n // tp
        idx = lax.axis_index('sp').astype(jnp.int32)
        cos, sin = rope_tables(pos, dh)
        xs = lax.dynamic_slice_in_dim(x, lax.axis_index('tp') * part, part, axis=0)
        own = [
            jnp.concatenate([k_hist[l].reshape(nh, kvl * dh), v_hist[l].reshape(nh, kvl * dh)], axis=0)
            for l in range(layers)
        ]
        near = to_neighbours(own[0])
        own_o = to_other(own[0])

        ks, vs = [], []
        for l in range(layers):
            if l == 0:
                h, own_o = after((rmsnorm(x, g1[l]), own_o))
            else:
                h = lax.all_gather(rmsnorm(xs, g1[l]), 'tp', axis=0, tiled=True)
            q, k, v = qkv(h, wq, wk, wv, l, cos, sin)
            ks.append(k.reshape(n, kvl, dh))
            vs.append(v.reshape(n, kvl, dh))
            kv_all = lax.all_gather(jnp.stack([k, v]), 'sp', axis=1, tiled=True)
            if l == 0:
                state = hist_attention(q, (), [own[l], *own_o], [], dh, kvl)
                near, state = after((near, tuple(state)))
                far = to_far(*near)
                near_o = to_other(*near)
                state = hist_attention(q, state, [*near, *near_o], [], dh, kvl)
                far, state = after((far, tuple(state)))
                far_o = to_other(*far)
                state = hist_attention(q, state, [], [*far, *far_o], dh, kvl)
            else:
                state = hist_attention(q, (), [own[l], *near, *own_o, *near_o], [*far, *far_o], dh, kvl)
            if l + 1 < layers:
                own[l + 1], _ = after((own[l + 1], far))
                near = to_neighbours(own[l + 1])
            attn = new_attention(idx.reshape(1), q, state, kv_all[0], kv_all[1], dh, kvl)
            if l + 1 < layers:
                attn, near = after((attn, near))
                far = to_far(*near)
            y = by_columns(down_kernel, attn, (wo,), l, 1024, jnp.float32, 'attn_out')
            y = lax.psum_scatter(y, 'tp', scatter_dimension=0, tiled=True)
            xs = xs + y.astype(jnp.bfloat16)

            h2 = lax.all_gather(rmsnorm(xs, g2[l]), 'tp', axis=0, tiled=True)
            if l + 1 < layers:
                h2, far = after((h2, far))
                own_o, near_o, far_o = to_other(own[l + 1]), to_other(*near), to_other(*far)
            u = by_columns(gate_kernel, h2, (wg, wu), l, 512, jnp.bfloat16, 'gate_up')
            if l + 1 < layers:
                u, own_o, near_o, far_o = after((u, own_o, near_o, far_o))
            y = by_columns(down_kernel, u, (wd,), l, 512, jnp.float32, 'down')
            y = lax.psum_scatter(y, 'tp', scatter_dimension=0, tiled=True)
            xs = xs + y.astype(jnp.bfloat16)
        x = lax.all_gather(xs, 'tp', axis=0, tiled=True)
        return x, jnp.stack(ks), jnp.stack(vs)

    in_specs = (P(row, None), P(row), kv_spec, kv_spec, col, col, col, rowsplit, col, col, rowsplit, P(), P())
    out_specs = (P(row, None), kv_spec, kv_spec)
    return jax.shard_map(body, mesh=mesh, in_specs=in_specs, out_specs=out_specs, check_vma=False)
```
